32 devices in a mesh: ka: 8 (over y, x, core), slab: 4 (over z).
Axes of the slice: x: 2, y: 2, z: 4, core: 2. Of those that a mesh axis runs over, the one named last changes fastest.
Arguments:
- val_wave: float32 [2, 8, 2, 12, 16, 128], P(None, 'ka', None, 'slab'), may hold values from -6 to 6
- cond_wave: float32 [2, 8, 8, 12, 16, 128], P(None, 'ka', None, 'slab'), may hold values from -6 to 6
- val_energy: float32 [8, 2], P('ka'), may hold values from -2 to -0.5
- cond_energy: float32 [8, 8], P('ka'), may hold values from 0.5 to 3
- frequency: float32 [4], replicated, may hold values from 0.2 to 4
- kpoint_map: int32 [8], replicated, may hold values from 0 to 7, as said below
- umklapp: int32 [3, 8], replicated, may hold values from 0 to 1, as said below
- gvector_index: int32 [6144], replicated, may hold values from 0 to 24575, as said below
Outputs:
- polarizability: float32 [4, 2, 6144, 6144], P(None, None, 'ka', 'slab')
The draws below stay inside these ranges and needn't reach their ends.
Inputs may be any that keep to these rules, and one draw needn't show every extreme that they name: With s the integer for which s * s * s = 8 and k = s * s * i + s * j + l, kpoint_map[k] is the index of (i + q0, j + q1, l + q2) taken modulo s in each coordinate, for one vector q whose components lie in 0 to s - 1, not all zero. umklapp[d, k] is 1 where coordinate d of k plus component d of q reaches s, else 0. `gvector_index`: entries are distinct.
All inputs are finite; a program needn't handle non-finite values.
Results may differ from the reference program's by a relative error of at most 0.0038.
Values may be sent and summed in bfloat16 or wider, within the bound.
A program may use at most 128 MiB of HBM per device.

```python
import math
import jax
import jax.numpy as jnp
from jax import lax

NV = 2
NC = 8
GX = 12
GY = 16
GZ = 128
NG = 6144
NW = 4
NK = 8
N_KA = 8


def grid_parts(key):
    grid_side = max((candidate for candidate in range(1, 9) if candidate ** 3 <= N_KA))
    flat_shift = jax.random.randint(jax.random.fold_in(key, 29), (), 1, grid_side ** 3)
    shift = [flat_shift // grid_side ** (2 - grid_dim) % grid_side for grid_dim in range(3)]
    index = jnp.arange(N_KA, dtype=jnp.int32)
    moved = [index // grid_side ** (2 - grid_dim) % grid_side + shift[grid_dim] for grid_dim in range(3)]
    mapped = sum((moved[grid_dim] % grid_side * grid_side ** (2 - grid_dim) for grid_dim in range(3)))
    folded = jnp.stack([(moved[grid_dim] >= grid_side).astype(jnp.int32) for grid_dim in range(3)])
    return (mapped.astype(jnp.int32), folded)


def draw_kpoint_map(key, part):
    return grid_parts(key)[0]


def draw_umklapp(key, part):
    return grid_parts(key)[1]


def draw_gvector_index(key, part):
    return jax.random.permutation(key, GX * GY * GZ)[:NG].astype(jnp.int32)


def block_levels(stream_key, shape, split, smallest, high):
    gain, own = 1.0, jax.random.fold_in(stream_key, 6)
    for position, shards_of in split:
        heights = jnp.exp(jax.random.uniform(jax.random.fold_in(own, position), (shards_of,), jnp.float32, smallest / len(split), high / len(split)))
        gain = gain * jnp.repeat(heights, shape[position] // shards_of).reshape([-1 if axis == position else 1 for axis in range(len(shape))])
    return gain


def gaussian(own_key, shape, spread, limit, cuts=(), held_as=jnp.bfloat16):
    level = block_levels(own_key, shape, cuts, -0.22, 0.18) if cuts else 1.0
    drawn = jax.random.normal(own_key, shape, jnp.float32) * spread * level
    return jnp.minimum(jnp.maximum(drawn, -limit), limit).astype(held_as)


def setup_inputs(seed: int = 0) -> dict:
    streams_of = jax.random.split(jax.random.key(seed), 9)
    return {
        "val_wave": gaussian(streams_of[0], (2, NK, NV, GX, GY, GZ), 1.0, 6.0, ((1, 8), (3, 4)), jnp.float32),
        "cond_wave": gaussian(streams_of[1], (2, NK, NC, GX, GY, GZ), 1.0, 6.0, ((1, 8), (3, 4)), jnp.float32),
        "val_energy": jnp.clip(-2.0 + 1.5 * jax.random.uniform(streams_of[2], (NK, NV), jnp.float32) ** block_levels(streams_of[2], (NK, NV), ((0, 8),), -0.2, 0.2), -2.0, -0.5),
        "cond_energy": jnp.clip(0.5 + 2.5 * jax.random.uniform(streams_of[3], (NK, NC), jnp.float32) ** block_levels(streams_of[3], (NK, NC), ((0, 8),), -0.2, 0.2), 0.5, 3.0),
        "frequency": jnp.clip(jnp.exp(jax.random.uniform(streams_of[4], (NW,), jnp.float32, math.log(0.2), math.log(4.0))), 0.2, 4.0),
        "kpoint_map": draw_kpoint_map(jax.random.fold_in(streams_of[8], 71), 0),
        "umklapp": draw_umklapp(jax.random.fold_in(streams_of[8], 71), 0),
        "gvector_index": draw_gvector_index(jax.random.fold_in(streams_of[8], 71), 0),
    }


two_pi = 2.0 * math.pi

def phase_angle(shift_vec, xpos, ypos, zpos):
    first_part = (shift_vec[0] * xpos % GX).astype(jnp.float32)[:, None, None] / GX
    second_part = (shift_vec[1] * ypos % GY).astype(jnp.float32)[None, :, None] / GY
    third_part = (shift_vec[2] * zpos % GZ).astype(jnp.float32)[None, None, :] / GZ
    return two_pi * (first_part + second_part + third_part)

def reference(val_wave, cond_wave, val_energy, cond_energy, frequency, kpoint_map, umklapp, gvector_index):
    pairs = NV * NC
    points = GX * GY * GZ
    kcount = val_wave.shape[1]
    xpos = jnp.arange(GX, dtype=jnp.int32)
    ypos = jnp.arange(GY, dtype=jnp.int32)
    zpos = jnp.arange(GZ, dtype=jnp.int32)
    norm = 1.0 / (2.0 * math.sqrt(points))

    def one_point(kpoint):
        valence = val_wave[:, kpoint]
        conduct = cond_wave[:, kpoint_map[kpoint]]
        angle = phase_angle(umklapp[:, kpoint], xpos, ypos, zpos)
        rotor = jnp.cos(angle) + 1j * jnp.sin(angle)
        cwave = (conduct[0] + 1j * conduct[1]) * rotor
        vwave = valence[0] + 1j * valence[1]
        density = (jnp.conj(vwave)[:, None] * cwave[None]).reshape(pairs, GX, GY, GZ)
        spectrum = jnp.fft.fftn(density, axes=(1, 2, 3)).reshape(pairs, points)[:, gvector_index] * norm
        return jnp.stack([jnp.real(spectrum), jnp.imag(spectrum)]).astype(jnp.float32)
    pair = lax.map(one_point, jnp.arange(kcount, dtype=jnp.int32))
    gap = (val_energy[:, :, None] - cond_energy[kpoint_map][:, None, :]).reshape(kcount, pairs)
    weight = 2.0 * gap[:, None, :] / (gap[:, None, :] ** 2 + frequency[None, :, None] ** 2) / kcount
    pair_low = lax.optimization_barrier(pair.astype(jnp.bfloat16)).astype(jnp.float32)
    right = jnp.concatenate([pair_low[:, 0].reshape(kcount * pairs, NG), pair_low[:, 1].reshape(kcount * pairs, NG)], 0)
    dims = (((0,), (0,)), ((), ()))

    def one_freq(weight_col):
        scaled = lax.optimization_barrier((pair * weight_col[:, None, :, None]).astype(jnp.bfloat16)).astype(jnp.float32)
        real_part = scaled[:, 0].reshape(kcount * pairs, NG)
        imag_part = scaled[:, 1].reshape(kcount * pairs, NG)
        left_re = jnp.concatenate([real_part, imag_part], 0)
        left_im = jnp.concatenate([imag_part, -real_part], 0)
        out_re = lax.dot_general(left_re, right, dims, preferred_element_type=jnp.float32)
        out_im = lax.dot_general(left_im, right, dims, preferred_element_type=jnp.float32)
        return jnp.stack([out_re, out_im])
    return lax.map(one_freq, jnp.transpose(weight, (1, 0, 2)))
```

```python
import functools
import math

import jax
import jax.numpy as jnp
import numpy as np
from jax import lax
from jax.experimental import pallas as pl
from jax.experimental.pallas import tpu as pltpu
from jax.sharding import PartitionSpec as P

two_pi = 2.0 * math.pi
f32 = jnp.float32
bf16 = jnp.bfloat16


def halves(table):
    high = table.astype(np.float32).astype(bf16)
    low = (table - high.astype(np.float64)).astype(np.float32).astype(bf16)
    return jnp.asarray(np.stack([high, low]))


def dft_angle(length):
    index = np.arange(length)
    return two_pi * (index[:, None] * index[None, :] % length) / length


def z_table(length):
    angle = dft_angle(length)
    cosine, sine = np.cos(angle), np.sin(angle)
    return halves(np.block([[cosine, sine], [-sine, cosine]]))


def plane_table(extent_x, extent_y):
    angle = np.kron(dft_angle(extent_x), np.ones((extent_y, extent_y))) + np.kron(
        np.ones((extent_x, extent_x)), dft_angle(extent_y)
    )
    return halves(np.cos(angle)), halves(np.sin(angle))


def split(value):
    high = value.astype(bf16)
    return high, (value - high.astype(f32)).astype(bf16)


def dot(a, b, dims):
    return lax.dot_general(a, b, (dims, ((), ())), preferred_element_type=f32)


def dot3(a, b, dims):
    return dot(a[0], b[0], dims) + dot(a[1], b[0], dims) + dot(a[0], b[1], dims)


def pair_kernel(norm, tile, val, cond, ztab, ctab, stab, gxy, gz, out, spectrum):
    bands_v, bands_c = val.shape[1], cond.shape[1]
    points, length = val.shape[2], val.shape[3]
    pairs = bands_v * bands_c
    ztable = (ztab[0], ztab[1])
    ctable = (ctab[0], ctab[1])
    stable = (stab[0], stab[1])
    for v in range(bands_v):
        for c in range(bands_c):
            p = v * bands_c + c
            re = val[0, v] * cond[0, c] + val[1, v] * cond[1, c]
            im = val[0, v] * cond[1, c] - val[1, v] * cond[0, c]
            field = split(jnp.concatenate([re, im], axis=1))
            along = split(dot3(ztable, field, ((1,), (1,))))
            even = dot3(along, ctable, ((1,), (0,)))
            odd = dot3(along, stable, ((1,), (0,)))
            real = (even[:length] + odd[length:]) * norm
            imag = (even[length:] - odd[:length]) * norm
            spectrum[pl.ds(p * length, length), :] = real.astype(bf16)
            spectrum[pl.ds((pairs + p) * length, length), :] = imag.astype(bf16)

    @pl.loop(0, out.shape[1] // tile)
    def _(step):
        cols = pl.ds(pl.multiple_of(step * tile, tile), tile)
        chosen = lax.broadcasted_iota(jnp.int32, (points, tile), 0) == gxy[:, cols]
        picked = dot(spectrum[...], chosen.astype(f32).astype(bf16), ((1,), (0,)))
        here = lax.broadcasted_iota(jnp.int32, (length, tile), 0) == gz[:, cols]
        rows = [
            jnp.sum(
                jnp.where(here, picked[r * length : (r + 1) * length], 0.0),
                axis=0,
                keepdims=True,
            )
            for r in range(2 * pairs)
        ]
        out[:, cols] = jnp.concatenate(rows, axis=0).astype(bf16)


def make_pairs(val, cond, gxy, gz, norm, tables):
    bands_v, bands_c = val.shape[1], cond.shape[1]
    points, length = val.shape[2], val.shape[3]
    total = gxy.shape[1]
    rows = 2 * bands_v * bands_c
    tile = 512 if total % 512 == 0 else 128
    vmem = pl.BlockSpec(memory_space=pltpu.VMEM)
    return pl.pallas_call(
        functools.partial(pair_kernel, norm, tile),
        out_shape=jax.ShapeDtypeStruct((rows, total), bf16),
        in_specs=[vmem] * 7,
        out_specs=vmem,
        scratch_shapes=[pltpu.VMEM((rows * length, points), bf16)],
        cost_estimate=pl.CostEstimate(
            flops=2 * rows * length * points * total, bytes_accessed=1 << 21, transcendentals=0
        ),
        name="pairs",
    )(val, cond, *tables, gxy, gz)


def product_kernel(tile, rows, cols, wsame, wswap, out, same, swap):
    @pl.when((pl.program_id(0) == 0) & (pl.program_id(1) == 0))
    def _():
        depth, width = rows.shape
        wide = rows[...].astype(f32)
        same[...] = wide.T
        group = wide.reshape(depth // 8, 8, width)
        turned = jnp.concatenate([group[:, 4:], group[:, :4]], axis=1)
        swap[...] = turned.reshape(depth, width).T

    step = pl.program_id(1)
    here = pl.ds(pl.multiple_of(step * tile, tile), tile)
    weight_same = wsame[pl.ds(pl.program_id(0), 1), :]
    weight_swap = wswap[pl.ds(pl.program_id(0), 1), :]
    right = cols[...]
    out[0, 0] = dot((same[here, :] * weight_same).astype(bf16), right, ((1,), (0,)))
    out[0, 1] = dot((swap[here, :] * weight_swap).astype(bf16), right, ((1,), (0,)))


def make_product(rows, cols, wsame, wswap):
    depth, height = rows.shape
    width = cols.shape[1]
    freqs = wsame.shape[0]
    tile = 128 if height % 128 == 0 else height
    vmem = pl.BlockSpec(memory_space=pltpu.VMEM)
    return pl.pallas_call(
        functools.partial(product_kernel, tile),
        out_shape=jax.ShapeDtypeStruct((freqs, 2, height, width), f32),
        grid=(freqs, height // tile),
        in_specs=[vmem] * 4,
        out_specs=pl.BlockSpec((1, 2, tile, width), lambda w, t: (w, 0, t, 0)),
        scratch_shapes=[pltpu.VMEM((height, depth), f32)] * 2,
        cost_estimate=pl.CostEstimate(
            flops=4 * freqs * depth * height * width,
            bytes_accessed=8 * freqs * height * width,
            transcendentals=0,
        ),
        name="product",
    )(rows, cols, wsame, wswap)


def route(payload, shift_flat, grid_side, count):
    for grid_dim in range(3):
        stride = grid_side ** (2 - grid_dim)
        for bit_pos in range(grid_side.bit_length() - 1):
            hop = 1 << bit_pos
            perm = []
            for source in range(count):
                coord = source // stride % grid_side
                perm.append((source, source + ((coord + hop) % grid_side - coord) * stride))
            moved = lax.ppermute(payload, "ka", perm)
            chosen = shift_flat // stride % grid_side // hop % 2 == 1
            payload = jnp.where(chosen, moved, payload)
    return payload


def per_device(
    val_wave, cond_wave, val_energy, cond_energy, frequency, kpoint_map, umklapp, gvector_index
):
    slab_count = lax.axis_size("slab")
    kpoint_count = lax.axis_size("ka")
    kpoint_here = lax.axis_index("ka")
    slab_here = lax.axis_index("slab")
    grid_side = max((candidate for candidate in range(1, 9) if candidate**3 <= kpoint_count))
    bands_v, planes, extent_y, extent_z = val_wave.shape[2:]
    bands_c = cond_wave.shape[2]
    extent_x = planes * slab_count
    local_c = bands_c // slab_count
    total_g = gvector_index.shape[0]
    points = extent_x * extent_y

    cond = lax.all_to_all(cond_wave[:, 0], "slab", split_axis=1, concat_axis=2, tiled=True)

    index = jnp.arange(kpoint_count, dtype=jnp.int32)
    shift_vec = jnp.sum(jnp.where(index[None, :] == kpoint_here, umklapp, 0), axis=1)
    xpos = slab_here * planes + jnp.arange(planes, dtype=jnp.int32)
    ypos = jnp.arange(extent_y, dtype=jnp.int32)
    zpos = jnp.arange(extent_z, dtype=jnp.int32)
    first_part = (shift_vec[0] * xpos % extent_x).astype(f32)[:, None, None] / extent_x
    second_part = (shift_vec[1] * ypos % extent_y).astype(f32)[None, :, None] / extent_y
    third_part = (shift_vec[2] * zpos % extent_z).astype(f32)[None, None, :] / extent_z
    angle = two_pi * (first_part + second_part + third_part)
    cosine = jnp.cos(angle)
    sine = jnp.sin(angle)
    val_re, val_im = val_wave[0, 0], val_wave[1, 0]
    turned = jnp.stack([val_re * cosine + val_im * sine, val_im * cosine - val_re * sine])
    routed = route(turned, kpoint_map[0], grid_side, kpoint_count)
    val = lax.all_gather(routed, "slab", axis=2, tiled=True)

    tables = (z_table(extent_z), *plane_table(extent_x, extent_y))
    norm = 1.0 / (2.0 * math.sqrt(points * extent_z))
    pair_low = make_pairs(
        val.reshape(2, bands_v, points, extent_z),
        cond.reshape(2, local_c, points, extent_z),
        (gvector_index // extent_z)[None],
        (gvector_index % extent_z)[None],
        norm,
        tables,
    )
    part = pair_low.shape[0]

    columns = lax.all_to_all(
        pair_low, "slab", split_axis=1, concat_axis=0, tiled=True
    )
    columns = lax.all_gather(columns, "ka", axis=0, tiled=True)
    rows = lax.all_to_all(
        pair_low.reshape(part, kpoint_count, total_g // kpoint_count),
        "ka", split_axis=1, concat_axis=0, tiled=True,
    ).reshape(kpoint_count, part, total_g // kpoint_count)
    rows = lax.all_gather(rows, "slab", axis=1, tiled=True)
    depth = kpoint_count * slab_count * part
    rows = rows.reshape(depth, total_g // kpoint_count)

    energies = lax.all_gather(
        jnp.concatenate([val_energy, cond_energy], axis=1), "ka", axis=0, tiled=True
    )
    came = kpoint_map[None, :] == index[:, None]
    val_level = jnp.sum(
        jnp.where(came[:, :, None], energies[None, :, :bands_v], 0.0), axis=1
    )
    cond_level = energies[:, bands_v:].reshape(kpoint_count, slab_count, 1, local_c)
    gap = val_level[:, None, :, None] - cond_level
    gap = gap.reshape(kpoint_count * slab_count, 1, bands_v * local_c)
    freq = frequency[:, None, None, None]
    weight = 2.0 * gap[None] / (gap[None] ** 2 + freq**2) / kpoint_count
    wsame = jnp.concatenate([weight, weight], axis=2).reshape(-1, depth)
    wswap = jnp.concatenate([weight, -weight], axis=2).reshape(-1, depth)
    return make_product(rows, columns, wsame, wswap)


def solution(mesh):
    return jax.shard_map(
        per_device,
        mesh=mesh,
        in_specs=(
            P(None, "ka", None, "slab", None, None),
            P(None, "ka", None, "slab", None, None),
            P("ka", None),
            P("ka", None),
            P(),
            P(),
            P(),
            P(),
        ),
        out_specs=P(None, None, "ka", "slab"),
        check_vma=False,
    )
```

```python
import functools
import math

import jax
import jax.numpy as jnp
import numpy as np
from jax import lax
from jax.experimental import pallas as pl
from jax.experimental.pallas import tpu as pltpu
from jax.sharding import PartitionSpec as P

two_pi = 2.0 * math.pi
f32 = jnp.float32
bf16 = jnp.bfloat16


def halves(table):
    high = table.astype(np.float32).astype(bf16)
    low = (table - high.astype(np.float64)).astype(np.float32).astype(bf16)
    return jnp.asarray(np.stack([high, low]))


def dft_angle(length):
    index = np.arange(length)
    return two_pi * (index[:, None] * index[None, :] % length) / length


def z_table(length):
    angle = dft_angle(length)
    cosine, sine = np.cos(angle), np.sin(angle)
    return halves(np.block([[cosine, sine], [-sine, cosine]]))


def plane_table(extent_x, extent_y):
    angle = np.kron(dft_angle(extent_x), np.ones((extent_y, extent_y))) + np.kron(
        np.ones((extent_x, extent_x)), dft_angle(extent_y)
    )
    return halves(np.cos(angle)), halves(np.sin(angle))


def split(value):
    high = value.astype(bf16)
    return high, (value - high.astype(f32)).astype(bf16)


def dot(a, b, dims):
    return lax.dot_general(a, b, (dims, ((), ())), preferred_element_type=f32)


def dot3(a, b, dims):
    return dot(a[0], b[0], dims) + dot(a[1], b[0], dims) + dot(a[0], b[1], dims)


def pair_kernel(norm, val, cond, ztab, ctab, stab, gxy, gz, out, spectrum):
    blocks, _, bands_v, _, length = val.shape
    bands_c = cond.shape[2]
    pairs = bands_v * bands_c
    points = spectrum.shape[1]
    tile = out.shape[2]
    ztable = (ztab[0], ztab[1])
    ctable = (ctab[0], ctab[1])
    stable = (stab[0], stab[1])
    for v in range(bands_v):
        for c in range(bands_c):
            p = v * bands_c + c
            pieces = []
            for b in range(blocks):
                val_re, val_im = val[b, 0, v], val[b, 1, v]
                cond_re, cond_im = cond[b, 0, c], cond[b, 1, c]
                re = val_re * cond_re + val_im * cond_im
                im = val_re * cond_im - val_im * cond_re
                pieces.append(jnp.concatenate([re, im], axis=1))
            field = split(jnp.concatenate(pieces, axis=0))
            along = split(dot3(ztable, field, ((1,), (1,))))
            even = dot3(along, ctable, ((1,), (0,)))
            odd = dot3(along, stable, ((1,), (0,)))
            real = (even[:length] + odd[length:]) * norm
            imag = (even[length:] - odd[:length]) * norm
            spectrum[pl.ds(p * length, length), :] = real.astype(bf16)
            spectrum[pl.ds((pairs + p) * length, length), :] = imag.astype(bf16)

    @pl.loop(0, out.shape[0])
    def _(step):
        cols = pl.ds(pl.multiple_of(step * tile, tile), tile)
        chosen = lax.broadcasted_iota(jnp.int32, (points, tile), 0) == gxy[:, cols]
        picked = dot(spectrum[...], chosen.astype(f32).astype(bf16), ((1,), (0,)))
        here = lax.broadcasted_iota(jnp.int32, (length, tile), 0) == gz[:, cols]
        rows = [
            jnp.sum(
                jnp.where(here, picked[r * length : (r + 1) * length], 0.0),
                axis=0,
                keepdims=True,
            )
            for r in range(2 * pairs)
        ]
        out[step] = jnp.concatenate(rows, axis=0).astype(bf16)


def make_pairs(val, cond, gxy, gz, tile, norm, tables):
    blocks, _, bands_v, rows, length = val.shape
    bands_c = cond.shape[2]
    points = blocks * rows
    total = gxy.shape[1]
    part = 2 * bands_v * bands_c
    vmem = pl.BlockSpec(memory_space=pltpu.VMEM)
    return pl.pallas_call(
        functools.partial(pair_kernel, norm),
        out_shape=jax.ShapeDtypeStruct((total // tile, part, tile), bf16),
        in_specs=[vmem] * 7,
        out_specs=vmem,
        scratch_shapes=[pltpu.VMEM((part * length, points), bf16)],
        cost_estimate=pl.CostEstimate(
            flops=2 * part * length * points * total, bytes_accessed=1 << 21, transcendentals=0
        ),
        name="pairs",
    )(val, cond, *tables, gxy, gz)


def meet(peers):
    barrier = pltpu.get_barrier_semaphore()
    for peer in peers:
        pl.semaphore_signal(barrier, inc=1, device_id=peer, device_id_type=pl.DeviceIdType.MESH)
    pl.semaphore_wait(barrier, len(peers))


def others(count_ka, count_slab):
    k, s = lax.axis_index("ka"), lax.axis_index("slab")
    along_ka = [(lax.rem(k + d, count_ka), s) for d in range(1, count_ka)]
    along_slab = [(k, lax.rem(s + d, count_slab)) for d in range(1, count_slab)]
    return k, s, along_ka, along_slab


def send(source, target, sems, number, peer):
    copy = pltpu.make_async_remote_copy(
        src_ref=source,
        dst_ref=target,
        send_sem=sems[0].at[number],
        recv_sem=sems[1].at[number],
        device_id=peer,
        device_id_type=pl.DeviceIdType.MESH,
    )
    copy.start()
    return copy


def keep(source, target, sem):
    copy = pltpu.make_async_copy(source, target, sem)
    copy.start()
    return copy


def spread_kernel(counts, val, cond, level, val_all, cond_all, level_all, sa, ra, sb, rb, sc, rc, own):
    k, s, along_ka, along_slab = others(*counts)
    meet(along_ka + along_slab)
    copies = []
    for i, peer in enumerate(along_ka):
        copies.append(send(val, val_all.at[k], (sa, ra), i, peer))
    for i, peer in enumerate(along_slab):
        copies.append(send(cond.at[peer[1]], cond_all.at[s], (sb, rb), i, peer))
    for i, peer in enumerate(along_ka):
        copies.append(send(level, level_all.at[k], (sc, rc), i, peer))
    copies.append(keep(val, val_all.at[k], own.at[0]))
    copies.append(keep(cond.at[s], cond_all.at[s], own.at[1]))
    copies.append(keep(level, level_all.at[k], own.at[2]))
    for copy in copies:
        copy.wait()


def gather_kernel(counts, val, val_all, sa, ra, own):
    k, s, _, along_slab = others(*counts)
    meet(along_slab)
    copies = [
        send(val, val_all.at[s], (sa, ra), i, peer) for i, peer in enumerate(along_slab)
    ]
    copies.append(keep(val, val_all.at[s], own.at[0]))
    for copy in copies:
        copy.wait()


def share_kernel(counts, tiles, blocks, cols_all, rows_all, sa, ra, sb, rb, sc, rc, sd, rd, own):
    k, s, along_ka, along_slab = others(*counts)
    per_column = cols_all.shape[0]
    meet(along_ka + along_slab)
    mine = [keep(blocks.at[k], rows_all.at[s, k], own.at[0])]
    mine.append(
        keep(tiles.at[pl.ds(s * per_column, per_column)], cols_all.at[:, s, k], own.at[1])
    )
    row_first = [
        send(blocks.at[peer[0]], rows_all.at[s, k], (sa, ra), i, peer)
        for i, peer in enumerate(along_ka)
    ]
    col_first = [
        send(
            tiles.at[pl.ds(peer[1] * per_column, per_column)],
            cols_all.at[:, s, k], (sb, rb), i, peer,
        )
        for i, peer in enumerate(along_slab)
    ]
    for copy in mine:
        copy.wait()
    for copy in row_first:
        copy.wait_recv()
    row_next = [
        send(rows_all.at[s], rows_all.at[s], (sc, rc), i, peer)
        for i, peer in enumerate(along_slab)
    ]
    for copy in col_first:
        copy.wait_recv()
    col_next = [
        send(cols_all.at[:, :, k], cols_all.at[:, :, k], (sd, rd), i, peer)
        for i, peer in enumerate(along_ka)
    ]
    for copy in row_first + col_first:
        copy.wait_send()
    for copy in row_next + col_next:
        copy.wait()


def exchange(body, name, number, counts, operands, outs, lanes):
    vmem = pl.BlockSpec(memory_space=pltpu.VMEM)
    sems = [pltpu.SemaphoreType.DMA((n - 1,)) for n in lanes for _ in range(2)]
    return pl.pallas_call(
        functools.partial(body, counts),
        out_shape=outs,
        in_specs=[vmem] * len(operands),
        out_specs=jax.tree.map(lambda _: vmem, outs),
        scratch_shapes=sems + [pltpu.SemaphoreType.DMA((3,))],
        compiler_params=pltpu.CompilerParams(collective_id=number, has_side_effects=True),
        name=name,
    )(*operands)


def product_kernel(tile, rows, cols, wsame, wswap, out, same, swap, right):
    @pl.when((pl.program_id(0) == 0) & (pl.program_id(1) == 0))
    def _():
        groups, part, width = rows.shape
        group = rows[...].astype(f32)
        same[...] = group.reshape(groups * part, width).T
        half = part // 2
        turned = jnp.concatenate([group[:, half:], group[:, :half]], axis=1)
        swap[...] = turned.reshape(groups * part, width).T
        wide = cols.shape[3]
        for j in range(cols.shape[0]):
            block = cols[j].astype(f32).reshape(groups * part, wide)
            right[:, pl.ds(j * wide, wide)] = block.astype(bf16)

    step = pl.program_id(1)
    here = pl.ds(pl.multiple_of(step * tile, tile), tile)
    weight_same = wsame[pl.ds(pl.program_id(0), 1), :]
    weight_swap = wswap[pl.ds(pl.program_id(0), 1), :]
    other = right[...]
    out[0, 0] = dot((same[here, :] * weight_same).astype(bf16), other, ((1,), (0,)))
    out[0, 1] = dot((swap[here, :] * weight_swap).astype(bf16), other, ((1,), (0,)))


def make_product(rows, cols, wsame, wswap):
    groups, part, height = rows.shape
    depth = groups * part
    width = cols.shape[0] * cols.shape[3]
    freqs = wsame.shape[0]
    tile = 128 if height % 128 == 0 else height
    vmem = pl.BlockSpec(memory_space=pltpu.VMEM)
    return pl.pallas_call(
        functools.partial(product_kernel, tile),
        out_shape=jax.ShapeDtypeStruct((freqs, 2, height, width), f32),
        grid=(freqs, height // tile),
        in_specs=[vmem] * 4,
        out_specs=pl.BlockSpec((1, 2, tile, width), lambda w, t: (w, 0, t, 0)),
        scratch_shapes=[pltpu.VMEM((height, depth), f32)] * 2
        + [pltpu.VMEM((depth, width), bf16)],
        cost_estimate=pl.CostEstimate(
            flops=4 * freqs * depth * height * width,
            bytes_accessed=8 * freqs * height * width,
            transcendentals=0,
        ),
        name="product",
    )(rows, cols, wsame, wswap)


def per_device(
    val_wave, cond_wave, val_energy, cond_energy, frequency, kpoint_map, umklapp, gvector_index
):
    slab_count = lax.axis_size("slab")
    kpoint_count = lax.axis_size("ka")
    kpoint_here = lax.axis_index("ka")
    slab_here = lax.axis_index("slab")
    grid_side = max((candidate for candidate in range(1, 9) if candidate**3 <= kpoint_count))
    bands_v, planes, extent_y, extent_z = val_wave.shape[2:]
    bands_c = cond_wave.shape[2]
    extent_x = planes * slab_count
    local_c = bands_c // slab_count
    total_g = gvector_index.shape[0]
    points = extent_x * extent_y

    index = jnp.arange(kpoint_count, dtype=jnp.int32)
    shift_vec = jnp.sum(jnp.where(index[None, :] == kpoint_here, umklapp, 0), axis=1)
    xpos = slab_here * planes + jnp.arange(planes, dtype=jnp.int32)
    ypos = jnp.arange(extent_y, dtype=jnp.int32)
    zpos = jnp.arange(extent_z, dtype=jnp.int32)
    first_part = (shift_vec[0] * xpos % extent_x).astype(f32)[:, None, None] / extent_x
    second_part = (shift_vec[1] * ypos % extent_y).astype(f32)[None, :, None] / extent_y
    third_part = (shift_vec[2] * zpos % extent_z).astype(f32)[None, None, :] / extent_z
    angle = two_pi * (first_part + second_part + third_part)
    cosine = jnp.cos(angle)
    sine = jnp.sin(angle)
    val_re, val_im = val_wave[0, 0], val_wave[1, 0]
    turned = jnp.stack([val_re * cosine + val_im * sine, val_im * cosine - val_re * sine])
    local = planes * extent_y
    val_out = turned.reshape(2, bands_v, local, extent_z)
    cond_out = cond_wave[:, 0]
    cond_out = jnp.swapaxes(
        cond_out.reshape(2, slab_count, local_c, local, extent_z), 0, 1
    )
    level = jnp.concatenate([val_energy, cond_energy], axis=1)
    level = jnp.pad(level, ((0, 7), (0, 128 - level.shape[1])))
    counts = (kpoint_count, slab_count)
    shape_of = jax.ShapeDtypeStruct
    val_all, cond, level_all = exchange(
        spread_kernel, "spread", 0, counts, (val_out, cond_out, level),
        (
            shape_of((kpoint_count, *val_out.shape), val_out.dtype),
            shape_of(cond_out.shape, cond_out.dtype),
            shape_of((kpoint_count, *level.shape), level.dtype),
        ),
        (kpoint_count, slab_count, kpoint_count),
    )
    came = kpoint_map[None, :] == index[:, None]
    source = jnp.sum(jnp.where(kpoint_map == kpoint_here, index, 0))
    val_here = lax.dynamic_index_in_dim(val_all, source, 0, keepdims=False)
    val = exchange(
        gather_kernel, "gather", 1, counts, (val_here,),
        shape_of((slab_count, *val_here.shape), val_here.dtype), (slab_count,),
    )

    tables = (z_table(extent_z), *plane_table(extent_x, extent_y))
    norm = 1.0 / (2.0 * math.sqrt(points * extent_z))
    column_g = total_g // slab_count
    row_g = total_g // kpoint_count
    tile = row_g if row_g % 128 == 0 and column_g % row_g == 0 else column_g
    tiles = make_pairs(
        val,
        cond,
        (gvector_index // extent_z)[None],
        (gvector_index % extent_z)[None],
        tile,
        norm,
        tables,
    )
    part = tiles.shape[1]
    blocks = tiles
    if tile != row_g:
        blocks = jnp.swapaxes(tiles, 0, 1).reshape(part, kpoint_count, row_g)
        blocks = jnp.swapaxes(blocks, 0, 1)
    columns, rows = exchange(
        share_kernel, "share", 2, counts, (tiles, blocks),
        (
            shape_of((column_g // tile, slab_count, kpoint_count, part, tile), bf16),
            shape_of((slab_count, kpoint_count, part, row_g), bf16),
        ),
        (kpoint_count, slab_count, slab_count, kpoint_count),
    )
    groups = slab_count * kpoint_count
    depth = groups * part

    energies = level_all[:, 0]
    val_level = jnp.sum(
        jnp.where(came[:, :, None], energies[None, :, :bands_v], 0.0), axis=1
    )
    cond_level = energies[:, bands_v : bands_v + bands_c]
    cond_level = jnp.swapaxes(cond_level.reshape(kpoint_count, slab_count, local_c), 0, 1)
    gap = val_level[None, :, :, None] - cond_level[:, :, None, :]
    gap = gap.reshape(groups, bands_v * local_c)
    freq = frequency[:, None, None]
    weight = 2.0 * gap[None] / (gap[None] ** 2 + freq**2) / kpoint_count
    wsame = jnp.concatenate([weight, weight], axis=2).reshape(-1, depth)
    wswap = jnp.concatenate([weight, -weight], axis=2).reshape(-1, depth)
    return make_product(
        rows.reshape(groups, part, row_g),
        columns.reshape(-1, groups, part, tile),
        wsame,
        wswap,
    )


def solution(mesh):
    return jax.shard_map(
        per_device,
        mesh=mesh,
        in_specs=(
            P(None, "ka", None, "slab", None, None),
            P(None, "ka", None, "slab", None, None),
            P("ka", None),
            P("ka", None),
            P(),
            P(),
            P(),
            P(),
        ),
        out_specs=P(None, None, "ka", "slab"),
        check_vma=False,
    )
```

```python
import functools
import math

import jax
import jax.numpy as jnp
import numpy as np
from jax import lax
from jax.experimental import pallas as pl
from jax.experimental.pallas import tpu as pltpu
from jax.sharding import PartitionSpec as P

two_pi = 2.0 * math.pi
f32 = jnp.float32
bf16 = jnp.bfloat16


def halves(table):
    high = table.astype(np.float32).astype(bf16)
    low = (table - high.astype(np.float64)).astype(np.float32).astype(bf16)
    return jnp.asarray(np.stack([high, low]))


def dft_angle(length):
    index = np.arange(length)
    return two_pi * (index[:, None] * index[None, :] % length) / length


def z_table(length):
    angle = dft_angle(length)
    cosine, sine = np.cos(angle), np.sin(angle)
    return halves(np.block([[cosine, sine], [-sine, cosine]]))


def plane_table(extent_x, extent_y):
    angle = np.kron(dft_angle(extent_x), np.ones((extent_y, extent_y))) + np.kron(
        np.ones((extent_x, extent_x)), dft_angle(extent_y)
    )
    return halves(np.cos(angle)), halves(np.sin(angle))


def split(value):
    high = value.astype(bf16)
    return high, (value - high.astype(f32)).astype(bf16)


def dot(a, b, dims):
    return lax.dot_general(a, b, (dims, ((), ())), preferred_element_type=f32)


def dot3(a, b, dims):
    return dot(a[0], b[0], dims) + dot(a[1], b[0], dims) + dot(a[0], b[1], dims)


def origin(kmap):
    here = lax.axis_index("ka")
    source = jnp.int32(0)
    for k in range(kmap.shape[0]):
        source = jnp.where(kmap[k] == here, k, source)
    return source


def pair_kernel(norm, extent_y, kmap, fold, val, cond, ztab, ctab, stab, gvec, out, spectrum):
    blocks, _, bands_v, _, length = val.shape
    bands_c = cond.shape[2]
    pairs = bands_v * bands_c
    points = spectrum.shape[1]
    tile = out.shape[2]
    ztable = (ztab[0], ztab[1])
    ctable = (ctab[0], ctab[1])
    stable = (stab[0], stab[1])
    for v in range(bands_v):
        for c in range(bands_c):
            p = v * bands_c + c
            pieces = []
            for b in range(blocks):
                val_re, val_im = val[b, 0, v], val[b, 1, v]
                cond_re, cond_im = cond[b, 0, c], cond[b, 1, c]
                re = val_re * cond_re + val_im * cond_im
                im = val_re * cond_im - val_im * cond_re
                pieces.append(jnp.concatenate([re, im], axis=1))
            field = split(jnp.concatenate(pieces, axis=0))
            along = split(dot3(ztable, field, ((1,), (1,))))
            even = dot3(along, ctable, ((1,), (0,)))
            odd = dot3(along, stable, ((1,), (0,)))
            real = (even[:length] + odd[length:]) * norm
            imag = (even[length:] - odd[:length]) * norm
            spectrum[pl.ds(p * length, length), :] = real.astype(bf16)
            spectrum[pl.ds((pairs + p) * length, length), :] = imag.astype(bf16)

    source = origin(kmap)
    extent_x = points // extent_y

    def moved(position, direction, extent):
        there = position - fold[direction, source]
        return jnp.where(there < 0, there + extent, there)

    @pl.loop(0, out.shape[0])
    def _(step):
        cols = pl.ds(pl.multiple_of(step * tile, tile), tile)
        index = gvec[:, cols]
        plane = lax.div(index, length)
        line_x = moved(lax.div(plane, extent_y), 0, extent_x)
        line_y = moved(lax.rem(plane, extent_y), 1, extent_y)
        gxy = line_x * extent_y + line_y
        gz = moved(lax.rem(index, length), 2, length)
        chosen = lax.broadcasted_iota(jnp.int32, (points, tile), 0) == gxy
        picked = dot(spectrum[...], chosen.astype(f32).astype(bf16), ((1,), (0,)))
        here = lax.broadcasted_iota(jnp.int32, (length, tile), 0) == gz
        rows = [
            jnp.sum(
                jnp.where(here, picked[r * length : (r + 1) * length], 0.0),
                axis=0,
                keepdims=True,
            )
            for r in range(2 * pairs)
        ]
        out[step] = jnp.concatenate(rows, axis=0).astype(bf16)


def make_pairs(kmap, fold, val, cond, gvec, extent_y, tile, norm, tables):
    blocks, _, bands_v, rows, length = val.shape
    bands_c = cond.shape[2]
    points = blocks * rows
    total = gvec.shape[1]
    part = 2 * bands_v * bands_c
    vmem = pl.BlockSpec(memory_space=pltpu.VMEM)
    smem = pl.BlockSpec(memory_space=pltpu.SMEM)
    return pl.pallas_call(
        functools.partial(pair_kernel, norm, extent_y),
        out_shape=jax.ShapeDtypeStruct((total // tile, part, tile), bf16),
        in_specs=[smem] * 2 + [vmem] * 6,
        out_specs=vmem,
        scratch_shapes=[pltpu.VMEM((part * length, points), bf16)],
        cost_estimate=pl.CostEstimate(
            flops=2 * part * length * points * total, bytes_accessed=1 << 21, transcendentals=0
        ),
        name="pairs",
    )(kmap, fold, val, cond, *tables, gvec)


def meet(peers):
    barrier = pltpu.get_barrier_semaphore()
    for peer in peers:
        pl.semaphore_signal(barrier, inc=1, device_id=peer, device_id_type=pl.DeviceIdType.MESH)
    pl.semaphore_wait(barrier, len(peers))


def others(count_ka, count_slab):
    k, s = lax.axis_index("ka"), lax.axis_index("slab")
    along_ka = [(lax.rem(k + d, count_ka), s) for d in range(1, count_ka)]
    along_slab = [(k, lax.rem(s + d, count_slab)) for d in range(1, count_slab)]
    return k, s, along_ka, along_slab


def send(source, target, sems, number, peer):
    copy = pltpu.make_async_remote_copy(
        src_ref=source,
        dst_ref=target,
        send_sem=sems[0].at[number],
        recv_sem=sems[1].at[number],
        device_id=peer,
        device_id_type=pl.DeviceIdType.MESH,
    )
    copy.start()
    return copy


def keep(source, target, sem):
    copy = pltpu.make_async_copy(source, target, sem)
    copy.start()
    return copy


def spread_kernel(
    counts, kmap, val, cond, level, val_all, cond_all, level_all,
    sa, ra, sb, rb, sc, rc, sd, rd, own, bank, staged,
):
    k, s, along_ka, along_slab = others(*counts)
    local_c = cond_all.shape[2]
    meet(along_ka + along_slab)
    to_ka = [send(val, bank.at[k], (sa, ra), i, peer) for i, peer in enumerate(along_ka)]
    rest = [
        send(cond.at[:, pl.ds(peer[1] * local_c, local_c)], cond_all.at[s], (sb, rb), i, peer)
        for i, peer in enumerate(along_slab)
    ]
    rest += [send(level, level_all.at[k], (sc, rc), i, peer) for i, peer in enumerate(along_ka)]
    keeps = [
        keep(val, bank.at[k], own.at[0]),
        keep(cond.at[:, pl.ds(s * local_c, local_c)], cond_all.at[s], own.at[1]),
        keep(level, level_all.at[k], own.at[2]),
    ]
    for copy in keeps:
        copy.wait()
    for copy in to_ka:
        copy.wait_recv()
    chosen = bank[origin(kmap)]
    staged[...] = chosen
    val_all[s] = chosen
    for copy in to_ka:
        copy.wait_send()
    to_slab = [
        send(staged, val_all.at[s], (sd, rd), i, peer) for i, peer in enumerate(along_slab)
    ]
    for copy in rest + to_slab:
        copy.wait()


def share_kernel(counts, tiles, blocks, cols_all, rows_all, sa, ra, sb, rb, sc, rc, sd, rd, own):
    k, s, along_ka, along_slab = others(*counts)
    per_column = cols_all.shape[0]
    meet(along_ka + along_slab)
    mine = [keep(blocks.at[k], rows_all.at[s, k], own.at[0])]
    mine.append(
        keep(tiles.at[pl.ds(s * per_column, per_column)], cols_all.at[:, s, k], own.at[1])
    )
    row_first = [
        send(blocks.at[peer[0]], rows_all.at[s, k], (sa, ra), i, peer)
        for i, peer in enumerate(along_ka)
    ]
    col_first = [
        send(
            tiles.at[pl.ds(peer[1] * per_column, per_column)],
            cols_all.at[:, s, k], (sb, rb), i, peer,
        )
        for i, peer in enumerate(along_slab)
    ]
    for copy in mine:
        copy.wait()
    for copy in row_first:
        copy.wait_recv()
    row_next = [
        send(rows_all.at[s], rows_all.at[s], (sc, rc), i, peer)
        for i, peer in enumerate(along_slab)
    ]
    for copy in col_first:
        copy.wait_recv()
    col_next = [
        send(cols_all.at[:, :, k], cols_all.at[:, :, k], (sd, rd), i, peer)
        for i, peer in enumerate(along_ka)
    ]
    for copy in row_first + col_first:
        copy.wait_send()
    for copy in row_next + col_next:
        copy.wait()


def exchange(body, name, number, counts, operands, outs, lanes, scratch=(), scalars=0):
    vmem = pl.BlockSpec(memory_space=pltpu.VMEM)
    smem = pl.BlockSpec(memory_space=pltpu.SMEM)
    sems = [pltpu.SemaphoreType.DMA((n - 1,)) for n in lanes for _ in range(2)]
    return pl.pallas_call(
        functools.partial(body, counts),
        out_shape=outs,
        in_specs=[smem] * scalars + [vmem] * (len(operands) - scalars),
        out_specs=jax.tree.map(lambda _: vmem, outs),
        scratch_shapes=sems + [pltpu.SemaphoreType.DMA((3,)), *scratch],
        compiler_params=pltpu.CompilerParams(collective_id=number, has_side_effects=True),
        name=name,
    )(*operands)


def product_kernel(tile, rows, cols, wsame, wswap, out, same, swap, right):
    @pl.when((pl.program_id(0) == 0) & (pl.program_id(1) == 0))
    def _():
        groups, part, width = rows.shape
        group = rows[...].astype(f32)
        same[...] = group.reshape(groups * part, width).T
        half = part // 2
        turned = jnp.concatenate([group[:, half:], group[:, :half]], axis=1)
        swap[...] = turned.reshape(groups * part, width).T
        wide = cols.shape[3]
        for j in range(cols.shape[0]):
            block = cols[j].astype(f32).reshape(groups * part, wide)
            right[:, pl.ds(j * wide, wide)] = block.astype(bf16)

    step = pl.program_id(1)
    here = pl.ds(pl.multiple_of(step * tile, tile), tile)
    weight_same = wsame[pl.ds(pl.program_id(0), 1), :]
    weight_swap = wswap[pl.ds(pl.program_id(0), 1), :]
    other = right[...]
    out[0, 0] = dot((same[here, :] * weight_same).astype(bf16), other, ((1,), (0,)))
    out[0, 1] = dot((swap[here, :] * weight_swap).astype(bf16), other, ((1,), (0,)))


def make_product(rows, cols, wsame, wswap):
    groups, part, height = rows.shape
    depth = groups * part
    width = cols.shape[0] * cols.shape[3]
    freqs = wsame.shape[0]
    tile = 128 if height % 128 == 0 else height
    vmem = pl.BlockSpec(memory_space=pltpu.VMEM)
    return pl.pallas_call(
        functools.partial(product_kernel, tile),
        out_shape=jax.ShapeDtypeStruct((freqs, 2, height, width), f32),
        grid=(freqs, height // tile),
        in_specs=[vmem] * 4,
        out_specs=pl.BlockSpec((1, 2, tile, width), lambda w, t: (w, 0, t, 0)),
        scratch_shapes=[pltpu.VMEM((height, depth), f32)] * 2
        + [pltpu.VMEM((depth, width), bf16)],
        cost_estimate=pl.CostEstimate(
            flops=4 * freqs * depth * height * width,
            bytes_accessed=8 * freqs * height * width,
            transcendentals=0,
        ),
        name="product",
    )(rows, cols, wsame, wswap)


def per_device(
    val_wave, cond_wave, val_energy, cond_energy, frequency, kpoint_map, umklapp, gvector_index
):
    slab_count = lax.axis_size("slab")
    kpoint_count = lax.axis_size("ka")
    bands_v, planes, extent_y, extent_z = val_wave.shape[2:]
    bands_c = cond_wave.shape[2]
    extent_x = planes * slab_count
    local_c = bands_c // slab_count
    total_g = gvector_index.shape[0]
    points = extent_x * extent_y

    index = jnp.arange(kpoint_count, dtype=jnp.int32)
    local = planes * extent_y
    val_out = val_wave.reshape(2, bands_v, local, extent_z)
    cond_out = cond_wave.reshape(2, bands_c, local, extent_z)
    level = jnp.concatenate([val_energy, cond_energy], axis=1)
    level = jnp.pad(level, ((0, 7), (0, 128 - level.shape[1])))
    counts = (kpoint_count, slab_count)
    shape_of = jax.ShapeDtypeStruct
    val, cond, level_all = exchange(
        spread_kernel, "spread", 0, counts, (kpoint_map, val_out, cond_out, level),
        (
            shape_of((slab_count, *val_out.shape), f32),
            shape_of((slab_count, 2, local_c, local, extent_z), f32),
            shape_of((kpoint_count, *level.shape), f32),
        ),
        (kpoint_count, slab_count, kpoint_count, slab_count),
        (
            pltpu.VMEM((kpoint_count, *val_out.shape), f32),
            pltpu.VMEM(val_out.shape, f32),
        ),
        1,
    )
    came = kpoint_map[None, :] == index[:, None]

    tables = (z_table(extent_z), *plane_table(extent_x, extent_y))
    norm = 1.0 / (2.0 * math.sqrt(points * extent_z))
    column_g = total_g // slab_count
    row_g = total_g // kpoint_count
    tile = row_g if row_g % 128 == 0 and column_g % row_g == 0 else column_g
    tiles = make_pairs(
        kpoint_map,
        umklapp,
        val,
        cond,
        gvector_index[None],
        extent_y,
        tile,
        norm,
        tables,
    )
    part = tiles.shape[1]
    blocks = tiles
    if tile != row_g:
        blocks = jnp.swapaxes(tiles, 0, 1).reshape(part, kpoint_count, row_g)
        blocks = jnp.swapaxes(blocks, 0, 1)
    columns, rows = exchange(
        share_kernel, "share", 1, counts, (tiles, blocks),
        (
            shape_of((column_g // tile, slab_count, kpoint_count, part, tile), bf16),
            shape_of((slab_count, kpoint_count, part, row_g), bf16),
        ),
        (kpoint_count, slab_count, slab_count, kpoint_count),
    )
    groups = slab_count * kpoint_count
    depth = groups * part

    energies = level_all[:, 0]
    val_level = jnp.sum(
        jnp.where(came[:, :, None], energies[None, :, :bands_v], 0.0), axis=1
    )
    cond_level = energies[:, bands_v : bands_v + bands_c]
    cond_level = jnp.swapaxes(cond_level.reshape(kpoint_count, slab_count, local_c), 0, 1)
    gap = val_level[None, :, :, None] - cond_level[:, :, None, :]
    gap = gap.reshape(groups, bands_v * local_c)
    freq = frequency[:, None, None]
    weight = 2.0 * gap[None] / (gap[None] ** 2 + freq**2) / kpoint_count
    wsame = jnp.concatenate([weight, weight], axis=2).reshape(-1, depth)
    wswap = jnp.concatenate([weight, -weight], axis=2).reshape(-1, depth)
    return make_product(
        rows.reshape(groups, part, row_g),
        columns.reshape(-1, groups, part, tile),
        wsame,
        wswap,
    )


def solution(mesh):
    return jax.shard_map(
        per_device,
        mesh=mesh,
        in_specs=(
            P(None, "ka", None, "slab", None, None),
            P(None, "ka", None, "slab", None, None),
            P("ka", None),
            P("ka", None),
            P(),
            P(),
            P(),
            P(),
        ),
        out_specs=P(None, None, "ka", "slab"),
        check_vma=False,
    )
```

```python
import functools
import math

import jax
import jax.numpy as jnp
import numpy as np
from jax import lax
from jax.experimental import pallas as pl
from jax.experimental.pallas import tpu as pltpu
from jax.sharding import PartitionSpec as P

two_pi = 2.0 * math.pi
f32 = jnp.float32
bf16 = jnp.bfloat16


def halves(table):
    high = table.astype(np.float32).astype(bf16)
    low = (table - high.astype(np.float64)).astype(np.float32).astype(bf16)
    return jnp.asarray(np.stack([high, low]))


def dft_angle(length):
    index = np.arange(length)
    return two_pi * (index[:, None] * index[None, :] % length) / length


def z_table(length):
    angle = dft_angle(length)
    cosine, sine = np.cos(angle), np.sin(angle)
    return halves(np.block([[cosine, sine], [-sine, cosine]]))


def plane_table(extent_x, extent_y):
    angle = np.kron(dft_angle(extent_x), np.ones((extent_y, extent_y))) + np.kron(
        np.ones((extent_x, extent_x)), dft_angle(extent_y)
    )
    return halves(np.cos(angle)), halves(np.sin(angle))


def split(value):
    high = value.astype(bf16)
    return high, (value - high.astype(f32)).astype(bf16)


def dot(a, b, dims):
    return lax.dot_general(a, b, (dims, ((), ())), preferred_element_type=f32)


def dot3(a, b, dims):
    return dot(a[0], b[0], dims) + dot(a[1], b[0], dims) + dot(a[0], b[1], dims)


def origin(kmap):
    here = lax.axis_index("ka")
    source = jnp.int32(0)
    for k in range(kmap.shape[0]):
        source = jnp.where(kmap[k] == here, k, source)
    return source


def pair_kernel(norm, extent_y, kmap, fold, val, cond, ztab, ctab, stab, gvec, out, spectrum):
    blocks, _, bands_v, _, length = val.shape
    bands_c = cond.shape[2]
    pairs = bands_v * bands_c
    points = spectrum.shape[1]
    tile = out.shape[2]
    ztable = (ztab[0], ztab[1])
    ctable = (ctab[0], ctab[1])
    stable = (stab[0], stab[1])
    for v in range(bands_v):
        for c in range(bands_c):
            p = v * bands_c + c
            pieces = []
            for b in range(blocks):
                val_re, val_im = val[b, 0, v], val[b, 1, v]
                cond_re, cond_im = cond[b, 0, c], cond[b, 1, c]
                re = val_re * cond_re + val_im * cond_im
                im = val_re * cond_im - val_im * cond_re
                pieces.append(jnp.concatenate([re, im], axis=1))
            field = split(jnp.concatenate(pieces, axis=0))
            along = split(dot3(ztable, field, ((1,), (1,))))
            even = dot3(along, ctable, ((1,), (0,)))
            odd = dot3(along, stable, ((1,), (0,)))
            real = (even[:length] + odd[length:]) * norm
            imag = (even[length:] - odd[:length]) * norm
            spectrum[pl.ds(p * length, length), :] = real.astype(bf16)
            spectrum[pl.ds((pairs + p) * length, length), :] = imag.astype(bf16)

    source = origin(kmap)
    extent_x = points // extent_y

    def moved(position, direction, extent):
        there = position - fold[direction, source]
        return jnp.where(there < 0, there + extent, there)

    @pl.loop(0, out.shape[0])
    def _(step):
        cols = pl.ds(pl.multiple_of(step * tile, tile), tile)
        index = gvec[:, cols]
        plane = lax.div(index, length)
        line_x = moved(lax.div(plane, extent_y), 0, extent_x)
        line_y = moved(lax.rem(plane, extent_y), 1, extent_y)
        gxy = line_x * extent_y + line_y
        gz = moved(lax.rem(index, length), 2, length)
        chosen = lax.broadcasted_iota(jnp.int32, (points, tile), 0) == gxy
        picked = dot(spectrum[...], chosen.astype(f32).astype(bf16), ((1,), (0,)))
        here = lax.broadcasted_iota(jnp.int32, (length, tile), 0) == gz
        rows = [
            jnp.sum(
                jnp.where(here, picked[r * length : (r + 1) * length], 0.0),
                axis=0,
                keepdims=True,
            )
            for r in range(2 * pairs)
        ]
        out[step] = jnp.concatenate(rows, axis=0).astype(bf16)


def make_pairs(kmap, fold, val, cond, gvec, extent_y, tile, norm, tables):
    blocks, _, bands_v, rows, length = val.shape
    bands_c = cond.shape[2]
    points = blocks * rows
    total = gvec.shape[1]
    part = 2 * bands_v * bands_c
    vmem = pl.BlockSpec(memory_space=pltpu.VMEM)
    smem = pl.BlockSpec(memory_space=pltpu.SMEM)
    return pl.pallas_call(
        functools.partial(pair_kernel, norm, extent_y),
        out_shape=jax.ShapeDtypeStruct((total // tile, part, tile), bf16),
        in_specs=[smem] * 2 + [vmem] * 6,
        out_specs=vmem,
        scratch_shapes=[pltpu.VMEM((part * length, points), bf16)],
        cost_estimate=pl.CostEstimate(
            flops=2 * part * length * points * total, bytes_accessed=1 << 21, transcendentals=0
        ),
        name="pairs",
    )(kmap, fold, val, cond, *tables, gvec)


def meet(peers):
    barrier = pltpu.get_barrier_semaphore()
    for peer in peers:
        pl.semaphore_signal(barrier, inc=1, device_id=peer, device_id_type=pl.DeviceIdType.MESH)
    pl.semaphore_wait(barrier, len(peers))


def others(count_ka, count_slab):
    k, s = lax.axis_index("ka"), lax.axis_index("slab")
    along_ka = [(lax.rem(k + d, count_ka), s) for d in range(1, count_ka)]
    along_slab = [(k, lax.rem(s + d, count_slab)) for d in range(1, count_slab)]
    return k, s, along_ka, along_slab


def send(source, target, sems, number, peer):
    copy = pltpu.make_async_remote_copy(
        src_ref=source,
        dst_ref=target,
        send_sem=sems[0].at[number],
        recv_sem=sems[1].at[number],
        device_id=peer,
        device_id_type=pl.DeviceIdType.MESH,
    )
    copy.start()
    return copy


def keep(source, target, sem):
    copy = pltpu.make_async_copy(source, target, sem)
    copy.start()
    return copy


def spread_kernel(
    counts, kmap, val, cond, level, val_all, cond_all, level_all,
    sa, ra, sb, rb, sc, rc, sd, rd, se, re, own, bank, staged,
):
    k, s, along_ka, along_slab = others(*counts)
    local_c = cond_all.shape[2]
    meet(along_ka + along_slab)
    count = counts[0]
    partner = (k + 1 - 2 * lax.rem(k, 2), s)
    steps = range(2, count, 2)
    to_ka = [
        send(val, bank.at[k], (sa, ra), i, (lax.rem(k + d, count), s))
        for i, d in enumerate(steps)
    ]
    to_partner = [send(val, bank.at[k], (se, re), 0, partner)]
    rest = [
        send(cond.at[:, pl.ds(peer[1] * local_c, local_c)], cond_all.at[s], (sb, rb), i, peer)
        for i, peer in enumerate(along_slab)
    ]
    rest += [send(level, level_all.at[k], (sc, rc), i, peer) for i, peer in enumerate(along_ka)]
    keeps = [
        keep(val, bank.at[k], own.at[0]),
        keep(cond.at[:, pl.ds(s * local_c, local_c)], cond_all.at[s], own.at[1]),
        keep(level, level_all.at[k], own.at[2]),
    ]
    for copy in keeps:
        copy.wait()
    for i, d in enumerate(steps):
        to_ka[i].wait_recv()
        block = bank.at[lax.rem(k + count - d, count)]
        to_partner.append(send(block, block, (se, re), i + 1, partner))
    for copy in to_partner:
        copy.wait_recv()
    chosen = bank[origin(kmap)]
    staged[...] = chosen
    val_all[s] = chosen
    for copy in to_ka + to_partner:
        copy.wait_send()
    to_slab = [
        send(staged, val_all.at[s], (sd, rd), i, peer) for i, peer in enumerate(along_slab)
    ]
    for copy in rest + to_slab:
        copy.wait()


def share_kernel(counts, tiles, blocks, cols_all, rows_all, sa, ra, sb, rb, sc, rc, sd, rd, own):
    k, s, along_ka, along_slab = others(*counts)
    per_column = cols_all.shape[0]
    meet(along_ka + along_slab)
    mine = [keep(blocks.at[k], rows_all.at[s, k], own.at[0])]
    mine.append(
        keep(tiles.at[pl.ds(s * per_column, per_column)], cols_all.at[:, s, k], own.at[1])
    )
    row_first = [
        send(blocks.at[peer[0]], rows_all.at[s, k], (sa, ra), i, peer)
        for i, peer in enumerate(along_ka)
    ]
    col_first = [
        send(
            tiles.at[pl.ds(peer[1] * per_column, per_column)],
            cols_all.at[:, s, k], (sb, rb), i, peer,
        )
        for i, peer in enumerate(along_slab)
    ]
    for copy in mine:
        copy.wait()
    for copy in row_first:
        copy.wait_recv()
    row_next = [
        send(rows_all.at[s], rows_all.at[s], (sc, rc), i, peer)
        for i, peer in enumerate(along_slab)
    ]
    for copy in col_first:
        copy.wait_recv()
    col_next = [
        send(cols_all.at[:, :, k], cols_all.at[:, :, k], (sd, rd), i, peer)
        for i, peer in enumerate(along_ka)
    ]
    for copy in row_first + col_first:
        copy.wait_send()
    for copy in row_next + col_next:
        copy.wait()


def exchange(body, name, number, counts, operands, outs, lanes, scratch=(), scalars=0):
    vmem = pl.BlockSpec(memory_space=pltpu.VMEM)
    smem = pl.BlockSpec(memory_space=pltpu.SMEM)
    sems = [pltpu.SemaphoreType.DMA((n - 1,)) for n in lanes for _ in range(2)]
    return pl.pallas_call(
        functools.partial(body, counts),
        out_shape=outs,
        in_specs=[smem] * scalars + [vmem] * (len(operands) - scalars),
        out_specs=jax.tree.map(lambda _: vmem, outs),
        scratch_shapes=sems + [pltpu.SemaphoreType.DMA((3,)), *scratch],
        compiler_params=pltpu.CompilerParams(collective_id=number, has_side_effects=True),
        name=name,
    )(*operands)


def product_kernel(tile, rows, cols, wsame, wswap, out, same, swap, right):
    @pl.when((pl.program_id(0) == 0) & (pl.program_id(1) == 0))
    def _():
        groups, part, width = rows.shape
        group = rows[...].astype(f32)
        same[...] = group.reshape(groups * part, width).T
        half = part // 2
        turned = jnp.concatenate([group[:, half:], group[:, :half]], axis=1)
        swap[...] = turned.reshape(groups * part, width).T
        wide = cols.shape[3]
        for j in range(cols.shape[0]):
            block = cols[j].astype(f32).reshape(groups * part, wide)
            right[:, pl.ds(j * wide, wide)] = block.astype(bf16)

    step = pl.program_id(1)
    here = pl.ds(pl.multiple_of(step * tile, tile), tile)
    weight_same = wsame[pl.ds(pl.program_id(0), 1), :]
    weight_swap = wswap[pl.ds(pl.program_id(0), 1), :]
    other = right[...]
    out[0, 0] = dot((same[here, :] * weight_same).astype(bf16), other, ((1,), (0,)))
    out[0, 1] = dot((swap[here, :] * weight_swap).astype(bf16), other, ((1,), (0,)))


def make_product(rows, cols, wsame, wswap):
    groups, part, height = rows.shape
    depth = groups * part
    width = cols.shape[0] * cols.shape[3]
    freqs = wsame.shape[0]
    tile = 128 if height % 128 == 0 else height
    vmem = pl.BlockSpec(memory_space=pltpu.VMEM)
    return pl.pallas_call(
        functools.partial(product_kernel, tile),
        out_shape=jax.ShapeDtypeStruct((freqs, 2, height, width), f32),
        grid=(freqs, height // tile),
        in_specs=[vmem] * 4,
        out_specs=pl.BlockSpec((1, 2, tile, width), lambda w, t: (w, 0, t, 0)),
        scratch_shapes=[pltpu.VMEM((height, depth), f32)] * 2
        + [pltpu.VMEM((depth, width), bf16)],
        cost_estimate=pl.CostEstimate(
            flops=4 * freqs * depth * height * width,
            bytes_accessed=8 * freqs * height * width,
            transcendentals=0,
        ),
        name="product",
    )(rows, cols, wsame, wswap)


def per_device(
    val_wave, cond_wave, val_energy, cond_energy, frequency, kpoint_map, umklapp, gvector_index
):
    slab_count = lax.axis_size("slab")
    kpoint_count = lax.axis_size("ka")
    bands_v, planes, extent_y, extent_z = val_wave.shape[2:]
    bands_c = cond_wave.shape[2]
    extent_x = planes * slab_count
    local_c = bands_c // slab_count
    total_g = gvector_index.shape[0]
    points = extent_x * extent_y

    index = jnp.arange(kpoint_count, dtype=jnp.int32)
    local = planes * extent_y
    val_out = val_wave.reshape(2, bands_v, local, extent_z)
    cond_out = cond_wave.reshape(2, bands_c, local, extent_z)
    level = jnp.concatenate([val_energy, cond_energy], axis=1)
    level = jnp.pad(level, ((0, 7), (0, 128 - level.shape[1])))
    counts = (kpoint_count, slab_count)
    shape_of = jax.ShapeDtypeStruct
    val, cond, level_all = exchange(
        spread_kernel, "spread", 0, counts, (kpoint_map, val_out, cond_out, level),
        (
            shape_of((slab_count, *val_out.shape), f32),
            shape_of((slab_count, 2, local_c, local, extent_z), f32),
            shape_of((kpoint_count, *level.shape), f32),
        ),
        (kpoint_count // 2, slab_count, kpoint_count, slab_count, kpoint_count // 2 + 1),
        (
            pltpu.VMEM((kpoint_count, *val_out.shape), f32),
            pltpu.VMEM(val_out.shape, f32),
        ),
        1,
    )
    came = kpoint_map[None, :] == index[:, None]

    tables = (z_table(extent_z), *plane_table(extent_x, extent_y))
    norm = 1.0 / (2.0 * math.sqrt(points * extent_z))
    column_g = total_g // slab_count
    row_g = total_g // kpoint_count
    tile = row_g if row_g % 128 == 0 and column_g % row_g == 0 else column_g
    tiles = make_pairs(
        kpoint_map,
        umklapp,
        val,
        cond,
        gvector_index[None],
        extent_y,
        tile,
        norm,
        tables,
    )
    part = tiles.shape[1]
    blocks = tiles
    if tile != row_g:
        blocks = jnp.swapaxes(tiles, 0, 1).reshape(part, kpoint_count, row_g)
        blocks = jnp.swapaxes(blocks, 0, 1)
    columns, rows = exchange(
        share_kernel, "share", 1, counts, (tiles, blocks),
        (
            shape_of((column_g // tile, slab_count, kpoint_count, part, tile), bf16),
            shape_of((slab_count, kpoint_count, part, row_g), bf16),
        ),
        (kpoint_count, slab_count, slab_count, kpoint_count),
    )
    groups = slab_count * kpoint_count
    depth = groups * part

    energies = level_all[:, 0]
    val_level = jnp.sum(
        jnp.where(came[:, :, None], energies[None, :, :bands_v], 0.0), axis=1
    )
    cond_level = energies[:, bands_v : bands_v + bands_c]
    cond_level = jnp.swapaxes(cond_level.reshape(kpoint_count, slab_count, local_c), 0, 1)
    gap = val_level[None, :, :, None] - cond_level[:, :, None, :]
    gap = gap.reshape(groups, bands_v * local_c)
    freq = frequency[:, None, None]
    weight = 2.0 * gap[None] / (gap[None] ** 2 + freq**2) / kpoint_count
    wsame = jnp.concatenate([weight, weight], axis=2).reshape(-1, depth)
    wswap = jnp.concatenate([weight, -weight], axis=2).reshape(-1, depth)
    return make_product(
        rows.reshape(groups, part, row_g),
        columns.reshape(-1, groups, part, tile),
        wsame,
        wswap,
    )


def solution(mesh):
    return jax.shard_map(
        per_device,
        mesh=mesh,
        in_specs=(
            P(None, "ka", None, "slab", None, None),
            P(None, "ka", None, "slab", None, None),
            P("ka", None),
            P("ka", None),
            P(),
            P(),
            P(),
            P(),
        ),
        out_specs=P(None, None, "ka", "slab"),
        check_vma=False,
    )
```

```python
import functools
import math

import jax
import jax.numpy as jnp
import numpy as np
from jax import lax
from jax.experimental import pallas as pl
from jax.experimental.pallas import tpu as pltpu
from jax.sharding import PartitionSpec as P

two_pi = 2.0 * math.pi
f32 = jnp.float32
bf16 = jnp.bfloat16


def halves(table):
    high = table.astype(np.float32).astype(bf16)
    low = (table - high.astype(np.float64)).astype(np.float32).astype(bf16)
    return jnp.asarray(np.stack([high, low]))


def dft_angle(length):
    index = np.arange(length)
    return two_pi * (index[:, None] * index[None, :] % length) / length


def z_table(length):
    angle = dft_angle(length)
    cosine, sine = np.cos(angle), np.sin(angle)
    return halves(np.block([[cosine, sine], [-sine, cosine]]))


def plane_table(extent_x, extent_y):
    angle = np.kron(dft_angle(extent_x), np.ones((extent_y, extent_y))) + np.kron(
        np.ones((extent_x, extent_x)), dft_angle(extent_y)
    )
    return halves(np.cos(angle)), halves(np.sin(angle))


def split(value):
    high = value.astype(bf16)
    return high, (value - high.astype(f32)).astype(bf16)


def dot(a, b, dims):
    return lax.dot_general(a, b, (dims, ((), ())), preferred_element_type=f32)


def dot3(a, b, dims):
    return dot(a[0], b[0], dims) + dot(a[1], b[0], dims) + dot(a[0], b[1], dims)


def origin(kmap):
    here = lax.axis_index("ka")
    source = jnp.int32(0)
    for k in range(kmap.shape[0]):
        source = jnp.where(kmap[k] == here, k, source)
    return source


def pair_kernel(norm, extent_y, kmap, fold, val, cond, ztab, ctab, stab, gvec, out, spectrum):
    blocks, _, bands_v, _, length = val.shape
    bands_c = cond.shape[2]
    pairs = bands_v * bands_c
    points = spectrum.shape[1]
    tile = out.shape[2]
    ztable = (ztab[0], ztab[1])
    ctable = (ctab[0], ctab[1])
    stable = (stab[0], stab[1])
    for v in range(bands_v):
        for c in range(bands_c):
            p = v * bands_c + c
            pieces = []
            for b in range(blocks):
                val_re, val_im = val[b, 0, v], val[b, 1, v]
                cond_re, cond_im = cond[b, 0, c], cond[b, 1, c]
                re = val_re * cond_re + val_im * cond_im
                im = val_re * cond_im - val_im * cond_re
                pieces.append(jnp.concatenate([re, im], axis=1))
            field = split(jnp.concatenate(pieces, axis=0))
            along = split(dot3(ztable, field, ((1,), (1,))))
            even = dot3(along, ctable, ((1,), (0,)))
            odd = dot3(along, stable, ((1,), (0,)))
            real = (even[:length] + odd[length:]) * norm
            imag = (even[length:] - odd[:length]) * norm
            spectrum[pl.ds(p * length, length), :] = real.astype(bf16)
            spectrum[pl.ds((pairs + p) * length, length), :] = imag.astype(bf16)

    source = origin(kmap)
    extent_x = points // extent_y

    def moved(position, direction, extent):
        there = position - fold[direction, source]
        return jnp.where(there < 0, there + extent, there)

    @pl.loop(0, out.shape[0])
    def _(step):
        cols = pl.ds(pl.multiple_of(step * tile, tile), tile)
        index = gvec[:, cols]
        plane = lax.div(index, length)
        line_x = moved(lax.div(plane, extent_y), 0, extent_x)
        line_y = moved(lax.rem(plane, extent_y), 1, extent_y)
        gxy = line_x * extent_y + line_y
        gz = moved(lax.rem(index, length), 2, length)
        chosen = lax.broadcasted_iota(jnp.int32, (points, tile), 0) == gxy
        picked = dot(spectrum[...], chosen.astype(f32).astype(bf16), ((1,), (0,)))
        here = lax.broadcasted_iota(jnp.int32, (length, tile), 0) == gz
        rows = [
            jnp.sum(
                jnp.where(here, picked[r * length : (r + 1) * length], 0.0),
                axis=0,
                keepdims=True,
            )
            for r in range(2 * pairs)
        ]
        out[step] = jnp.concatenate(rows, axis=0).astype(bf16)


def make_pairs(kmap, fold, val, cond, gvec, extent_y, tile, norm, tables):
    blocks, _, bands_v, rows, length = val.shape
    bands_c = cond.shape[2]
    points = blocks * rows
    total = gvec.shape[1]
    part = 2 * bands_v * bands_c
    vmem = pl.BlockSpec(memory_space=pltpu.VMEM)
    smem = pl.BlockSpec(memory_space=pltpu.SMEM)
    return pl.pallas_call(
        functools.partial(pair_kernel, norm, extent_y),
        out_shape=jax.ShapeDtypeStruct((total // tile, part, tile), bf16),
        in_specs=[smem] * 2 + [vmem] * 6,
        out_specs=vmem,
        scratch_shapes=[pltpu.VMEM((part * length, points), bf16)],
        cost_estimate=pl.CostEstimate(
            flops=2 * part * length * points * total, bytes_accessed=1 << 21, transcendentals=0
        ),
        name="pairs",
    )(kmap, fold, val, cond, *tables, gvec)


def meet(peers):
    barrier = pltpu.get_barrier_semaphore()
    for peer in peers:
        pl.semaphore_signal(barrier, inc=1, device_id=peer, device_id_type=pl.DeviceIdType.MESH)
    pl.semaphore_wait(barrier, len(peers))


def others(count_ka, count_slab):
    k, s = lax.axis_index("ka"), lax.axis_index("slab")
    along_ka = [(lax.rem(k + d, count_ka), s) for d in range(1, count_ka)]
    along_slab = [(k, lax.rem(s + d, count_slab)) for d in range(1, count_slab)]
    return k, s, along_ka, along_slab


def send(source, target, sems, number, peer):
    copy = pltpu.make_async_remote_copy(
        src_ref=source,
        dst_ref=target,
        send_sem=sems[0].at[number],
        recv_sem=sems[1].at[number],
        device_id=peer,
        device_id_type=pl.DeviceIdType.MESH,
    )
    copy.start()
    return copy


def keep(source, target, sem):
    copy = pltpu.make_async_copy(source, target, sem)
    copy.start()
    return copy


def spread_kernel(
    counts, kmap, val, cond, level, val_all, cond_all, level_all,
    sa, ra, sb, rb, sc, rc, sd, rd, se, re, own, bank, staged,
):
    k, s, along_ka, along_slab = others(*counts)
    local_c = cond_all.shape[2]
    meet(along_ka + along_slab)
    count = counts[0]
    partner = (k + 1 - 2 * lax.rem(k, 2), s)
    steps = range(2, count, 2)
    to_ka = [
        send(val, bank.at[k], (sa, ra), i, (lax.rem(k + d, count), s))
        for i, d in enumerate(steps)
    ]
    to_partner = [send(val, bank.at[k], (se, re), 0, partner)]
    rest = [
        send(cond.at[:, pl.ds(peer[1] * local_c, local_c)], cond_all.at[s], (sb, rb), i, peer)
        for i, peer in enumerate(along_slab)
    ]
    rest += [send(level, level_all.at[k], (sc, rc), i, peer) for i, peer in enumerate(along_ka)]
    keeps = [
        keep(val, bank.at[k], own.at[0]),
        keep(cond.at[:, pl.ds(s * local_c, local_c)], cond_all.at[s], own.at[1]),
        keep(level, level_all.at[k], own.at[2]),
    ]
    for copy in keeps:
        copy.wait()
    for i, d in enumerate(steps):
        to_ka[i].wait_recv()
        block = bank.at[lax.rem(k + count - d, count)]
        to_partner.append(send(block, block, (se, re), i + 1, partner))
    for copy in to_partner:
        copy.wait_recv()
    chosen = bank[origin(kmap)]
    staged[...] = chosen
    val_all[s] = chosen
    for copy in to_ka + to_partner:
        copy.wait_send()
    to_slab = [
        send(staged, val_all.at[s], (sd, rd), i, peer) for i, peer in enumerate(along_slab)
    ]
    for copy in rest + to_slab:
        copy.wait()


def share_kernel(counts, tiles, blocks, cols_all, rows_all, sa, ra, sb, rb, sc, rc, sd, rd, se, re, own):
    k, s, along_ka, along_slab = others(*counts)
    per_column = cols_all.shape[0]
    meet(along_ka + along_slab)
    mine = [keep(blocks.at[k], rows_all.at[s, k], own.at[0])]
    mine.append(
        keep(tiles.at[pl.ds(s * per_column, per_column)], cols_all.at[:, s, k], own.at[1])
    )
    row_first = [
        send(blocks.at[peer[0]], rows_all.at[s, k], (sa, ra), i, peer)
        for i, peer in enumerate(along_ka)
    ]
    col_first = [
        send(
            tiles.at[pl.ds(peer[1] * per_column, per_column)],
            cols_all.at[:, s, k], (sb, rb), i, peer,
        )
        for i, peer in enumerate(along_slab)
    ]
    for copy in mine:
        copy.wait()
    for copy in row_first:
        copy.wait_recv()
    row_next = [
        send(rows_all.at[s], rows_all.at[s], (sc, rc), i, peer)
        for i, peer in enumerate(along_slab)
    ]
    for copy in col_first:
        copy.wait_recv()
    count = counts[0]
    partner = (k + 1 - 2 * lax.rem(k, 2), s)
    steps = range(2, count, 2)
    block = cols_all.at[:, :, k]
    col_next = [
        send(block, block, (sd, rd), i, (lax.rem(k + d, count), s)) for i, d in enumerate(steps)
    ]
    to_partner = [send(block, block, (se, re), 0, partner)]
    for i, d in enumerate(steps):
        col_next[i].wait_recv()
        block = cols_all.at[:, :, lax.rem(k + count - d, count)]
        to_partner.append(send(block, block, (se, re), i + 1, partner))
    for copy in col_next:
        copy.wait_send()
    for copy in row_first + col_first:
        copy.wait_send()
    for copy in row_next + to_partner:
        copy.wait()


def exchange(body, name, number, counts, operands, outs, lanes, scratch=(), scalars=0):
    vmem = pl.BlockSpec(memory_space=pltpu.VMEM)
    smem = pl.BlockSpec(memory_space=pltpu.SMEM)
    sems = [pltpu.SemaphoreType.DMA((n - 1,)) for n in lanes for _ in range(2)]
    return pl.pallas_call(
        functools.partial(body, counts),
        out_shape=outs,
        in_specs=[smem] * scalars + [vmem] * (len(operands) - scalars),
        out_specs=jax.tree.map(lambda _: vmem, outs),
        scratch_shapes=sems + [pltpu.SemaphoreType.DMA((3,)), *scratch],
        compiler_params=pltpu.CompilerParams(collective_id=number, has_side_effects=True),
        name=name,
    )(*operands)


def product_kernel(tile, rows, cols, wsame, out, same, swap, right):
    @pl.when((pl.program_id(0) == 0) & (pl.program_id(1) == 0))
    def _():
        groups, part, width = rows.shape
        group = rows[...].astype(f32)
        same[...] = group.reshape(groups * part, width).T
        half = part // 2
        turned = jnp.concatenate([group[:, half:], group[:, :half]], axis=1)
        swap[...] = turned.reshape(groups * part, width).T
        wide = cols.shape[3]
        for j in range(cols.shape[0]):
            block = cols[j].astype(f32).reshape(groups * part, wide)
            right[:, pl.ds(j * wide, wide)] = block.astype(bf16)

    step = pl.program_id(1)
    here = pl.ds(pl.multiple_of(step * tile, tile), tile)
    weight_same = wsame[pl.ds(pl.program_id(0), 1), :]
    part = rows.shape[1]
    lane = lax.broadcasted_iota(jnp.int32, weight_same.shape, 1)
    weight_swap = jnp.where(lax.rem(lane, part) < part // 2, weight_same, -weight_same)
    other = right[...]
    out[0, 0] = dot((same[here, :] * weight_same).astype(bf16), other, ((1,), (0,)))
    out[0, 1] = dot((swap[here, :] * weight_swap).astype(bf16), other, ((1,), (0,)))


def make_product(rows, cols, wsame):
    groups, part, height = rows.shape
    depth = groups * part
    width = cols.shape[0] * cols.shape[3]
    freqs = wsame.shape[0]
    tile = 128 if height % 128 == 0 else height
    vmem = pl.BlockSpec(memory_space=pltpu.VMEM)
    return pl.pallas_call(
        functools.partial(product_kernel, tile),
        out_shape=jax.ShapeDtypeStruct((freqs, 2, height, width), f32),
        grid=(freqs, height // tile),
        in_specs=[vmem] * 3,
        out_specs=pl.BlockSpec((1, 2, tile, width), lambda w, t: (w, 0, t, 0)),
        scratch_shapes=[pltpu.VMEM((height, depth), f32)] * 2
        + [pltpu.VMEM((depth, width), bf16)],
        cost_estimate=pl.CostEstimate(
            flops=4 * freqs * depth * height * width,
            bytes_accessed=8 * freqs * height * width,
            transcendentals=0,
        ),
        name="product",
    )(rows, cols, wsame)


def per_device(
    val_wave, cond_wave, val_energy, cond_energy, frequency, kpoint_map, umklapp, gvector_index
):
    slab_count = lax.axis_size("slab")
    kpoint_count = lax.axis_size("ka")
    bands_v, planes, extent_y, extent_z = val_wave.shape[2:]
    bands_c = cond_wave.shape[2]
    extent_x = planes * slab_count
    local_c = bands_c // slab_count
    total_g = gvector_index.shape[0]
    points = extent_x * extent_y

    index = jnp.arange(kpoint_count, dtype=jnp.int32)
    local = planes * extent_y
    val_out = val_wave.reshape(2, bands_v, local, extent_z)
    cond_out = cond_wave.reshape(2, bands_c, local, extent_z)
    level = jnp.concatenate([val_energy, cond_energy], axis=1)
    level = jnp.pad(level, ((0, 7), (0, 128 - level.shape[1])))
    counts = (kpoint_count, slab_count)
    shape_of = jax.ShapeDtypeStruct
    val, cond, level_all = exchange(
        spread_kernel, "spread", 0, counts, (kpoint_map, val_out, cond_out, level),
        (
            shape_of((slab_count, *val_out.shape), f32),
            shape_of((slab_count, 2, local_c, local, extent_z), f32),
            shape_of((kpoint_count, *level.shape), f32),
        ),
        (kpoint_count // 2, slab_count, kpoint_count, slab_count, kpoint_count // 2 + 1),
        (
            pltpu.VMEM((kpoint_count, *val_out.shape), f32),
            pltpu.VMEM(val_out.shape, f32),
        ),
        1,
    )
    came = kpoint_map[None, :] == index[:, None]

    tables = (z_table(extent_z), *plane_table(extent_x, extent_y))
    norm = 1.0 / (2.0 * math.sqrt(points * extent_z))
    column_g = total_g // slab_count
    row_g = total_g // kpoint_count
    tile = row_g if row_g % 128 == 0 and column_g % row_g == 0 else column_g
    tiles = make_pairs(
        kpoint_map,
        umklapp,
        val,
        cond,
        gvector_index[None],
        extent_y,
        tile,
        norm,
        tables,
    )
    part = tiles.shape[1]
    blocks = tiles
    if tile != row_g:
        blocks = jnp.swapaxes(tiles, 0, 1).reshape(part, kpoint_count, row_g)
        blocks = jnp.swapaxes(blocks, 0, 1)
    columns, rows = exchange(
        share_kernel, "share", 1, counts, (tiles, blocks),
        (
            shape_of((column_g // tile, slab_count, kpoint_count, part, tile), bf16),
            shape_of((slab_count, kpoint_count, part, row_g), bf16),
        ),
        (kpoint_count, slab_count, slab_count, kpoint_count // 2, kpoint_count // 2 + 1),
    )
    groups = slab_count * kpoint_count
    depth = groups * part

    energies = level_all[:, 0]
    val_level = jnp.sum(
        jnp.where(came[:, :, None], energies[None, :, :bands_v], 0.0), axis=1
    )
    cond_level = energies[:, bands_v : bands_v + bands_c]
    cond_level = jnp.swapaxes(cond_level.reshape(kpoint_count, slab_count, local_c), 0, 1)
    gap = val_level[None, :, :, None] - cond_level[:, :, None, :]
    gap = gap.reshape(groups, bands_v * local_c)
    freq = frequency[:, None, None]
    weight = 2.0 * gap[None] / (gap[None] ** 2 + freq**2) / kpoint_count
    wsame = jnp.concatenate([weight, weight], axis=2).reshape(-1, depth)
    return make_product(
        rows.reshape(groups, part, row_g),
        columns.reshape(-1, groups, part, tile),
        wsame,
    )


def solution(mesh):
    return jax.shard_map(
        per_device,
        mesh=mesh,
        in_specs=(
            P(None, "ka", None, "slab", None, None),
            P(None, "ka", None, "slab", None, None),
            P("ka", None),
            P("ka", None),
            P(),
            P(),
            P(),
            P(),
        ),
        out_specs=P(None, None, "ka", "slab"),
        check_vma=False,
    )
```
